256 devices in a mesh: px: 32 (over y, z_hi, core), py: 8 (over z_lo, x).
Axes of the slice: x: 4, y: 4, z: 8 (z_hi: 4, z_lo: 2; z = z_hi * 2 + z_lo), core: 2. Of those that a mesh axis runs over, the one named last changes fastest.
Arguments:
- charges_old: float32 [32, 8, 32, 32, 512], P('px', 'py'), may hold values from -0.0026758191 to 0.0026758191
- spline_moduli: float32 [3, 512], replicated, may hold values from 1 to 2.5
Outputs:
- structure: float32 [2, 512, 512, 512], P(None, 'px', 'py')
- energy: float32 [], replicated
- virial: float32 [6], replicated
The draws below stay inside these ranges and needn't reach their ends.
All inputs are finite; a program needn't handle non-finite values.
Results may differ from the reference program's by a relative error of at most 0.0007.
Values sent between devices are 32-bit elements; how exact they have to be, the bound alone decides.
No kernel may reach another device: no remote copies, remote signals or barrier semaphores. Data moves between devices by JAX's collectives and lax.ppermute only.
A program may use at most 128 MiB of HBM per device.

```python
import math
import jax
import jax.numpy as jnp
from jax import lax

GRID = 512
PENCIL_ROWS = 32
PENCIL_COLS = 8
OLD_BX = 32
OLD_BY = 32


def draw_charges_old(key, part):
    key_list = jax.random.split(key, 3)
    full_shape = (PENCIL_ROWS, PENCIL_COLS, OLD_BX, OLD_BY, GRID)
    log_ten = math.log(10.0)
    row_scale = jnp.exp(jax.random.uniform(key_list[0], (GRID,), jnp.float32) * log_ten)
    col_scale = jnp.exp(jax.random.uniform(key_list[1], (GRID,), jnp.float32) * log_ten)
    pencil_row = jnp.arange(PENCIL_ROWS, dtype=jnp.int32).reshape(PENCIL_ROWS, 1, 1, 1, 1)
    pencil_col = jnp.arange(PENCIL_COLS, dtype=jnp.int32).reshape(1, PENCIL_COLS, 1, 1, 1)
    inner_row = jnp.arange(OLD_BX, dtype=jnp.int32).reshape(1, 1, OLD_BX, 1, 1)
    inner_col = jnp.arange(OLD_BY, dtype=jnp.int32).reshape(1, 1, 1, OLD_BY, 1)
    x_position = pencil_row // 2 * OLD_BX + inner_row
    y_position = (pencil_row % 2 * PENCIL_COLS + pencil_col) * OLD_BY + inner_col
    noise_field = jnp.clip(jax.random.normal(key_list[2], full_shape, jnp.float32), -6.0, 6.0)
    values = noise_field * row_scale[x_position] * col_scale[y_position]
    return values / (20.0 * GRID ** 1.5)


def setup_inputs(seed: int = 0) -> dict:
    streams_of = jax.random.split(jax.random.key(seed), 3)
    return {
        "charges_old": draw_charges_old(jax.random.fold_in(streams_of[2], 71), 0),
        "spline_moduli": jnp.clip(jnp.exp(jax.random.uniform(streams_of[1], (3, GRID), jnp.float32, math.log(1.0), math.log(2.5))), 1.0, 2.5),
    }


beta_nm = 3.12
cell_nm = 0.1


def signed_wave(mode_index, points):
    shifted = mode_index - points * (mode_index >= points // 2).astype(jnp.int32)
    return shifted.astype(jnp.float32) / (cell_nm * points)


def mode_sums(real_part, imag_part, wave_y, wave_z, wave_x, moduli_y, moduli_z, moduli_x, points):
    m_square = wave_y * wave_y + wave_z * wave_z + wave_x * wave_x
    anchor = m_square == 0.0
    safe_msq = jnp.where(anchor, 1.0, m_square)
    volume = (cell_nm * points) ** 3
    decay_ratio = (math.pi ** 2 / beta_nm ** 2) * m_square
    influence = jnp.exp(-decay_ratio) / (math.pi * volume * safe_msq) * moduli_y * moduli_z * moduli_x
    influence = jnp.where(anchor, 0.0, influence)
    mode_power = influence * (real_part * real_part + imag_part * imag_part)
    energy = 0.5 * jnp.sum(mode_power)
    weight = mode_power * (1.0 + decay_ratio) / safe_msq
    pair_sums = jnp.stack([
        jnp.sum(weight * wave_x * wave_x),
        jnp.sum(weight * wave_y * wave_y),
        jnp.sum(weight * wave_z * wave_z),
        jnp.sum(weight * wave_x * wave_y),
        jnp.sum(weight * wave_x * wave_z),
        jnp.sum(weight * wave_y * wave_z),
    ])
    return energy, pair_sums


def reference(charges_old, spline_moduli):
    points = GRID
    blocks = charges_old.reshape(PENCIL_ROWS // 2, 2, PENCIL_COLS, OLD_BX, OLD_BY, points)
    charge_mesh = blocks.transpose(0, 3, 1, 2, 4, 5).reshape(points, points, points)
    spectrum = jnp.transpose(jnp.fft.fftn(charge_mesh), (1, 2, 0))
    real_part = jnp.real(spectrum)
    imag_part = jnp.imag(spectrum)
    mode_index = jnp.arange(points, dtype=jnp.int32)
    wave_numbers = signed_wave(mode_index, points)
    wave_z = wave_numbers[:, None]
    wave_x = wave_numbers[None, :]
    moduli_z = spline_moduli[2][:, None]
    moduli_x = spline_moduli[0][None, :]

    def per_plane(plane_items):
        real_plane, imag_plane, wave_plane, moduli_plane = plane_items
        return mode_sums(real_plane, imag_plane, wave_plane, wave_z, wave_x, moduli_plane, moduli_z, moduli_x, points)

    energies, pair_sums = lax.map(per_plane, (real_part, imag_part, wave_numbers, spline_moduli[1]))
    energy = jnp.sum(energies)
    virial = energy * jnp.array([1.0, 1.0, 1.0, 0.0, 0.0, 0.0], dtype=jnp.float32) - jnp.sum(pair_sums, axis=0)
    structure = jnp.stack([real_part, imag_part])
    return structure, energy, virial
```

```python
import math

import jax
import jax.numpy as jnp
import numpy as np
from jax import lax
from jax.experimental import pallas as pl
from jax.experimental.pallas import tpu as pltpu
from jax.sharding import Mesh
from jax.sharding import PartitionSpec as P

PX = ("px_0", "px_1", "px_2")
PY = ("py_0", "py_1")
ALL = ("px_0", "px_1", "px_2", "py_0", "py_1")
FIRST = ("px_2", "py_0", "py_1")

GRID = 512
beta_nm = 3.12
cell_nm = 0.1
RATE = math.pi**2 / beta_nm**2
VOLUME = (cell_nm * GRID) ** 3
ROWS_A = 10
ROWS_B = 6
STEP = 2
EXT = 264
f32 = jnp.float32
bf16 = jnp.bfloat16


def split_table(table):
    high = table.astype(bf16)
    low = (table - high.astype(np.float64)).astype(bf16)
    return high, low


def z_table():
    z = np.arange(GRID)[:, None]
    column = np.arange(GRID)[None, :]
    kz = column // 64 * 32 + column % 32
    part = column // 32 % 2
    lane = np.arange(128)[None, :]
    kz = np.concatenate([kz, (lane % 8 + 1) * 32], axis=1)
    part = np.concatenate([part, lane // 32 % 2], axis=1)
    angle = z * kz % GRID * (2.0 * np.pi / GRID)
    return split_table(np.where(part == 0, np.cos(angle), -np.sin(angle)))


def circle(turns):
    angle = turns % GRID * (2.0 * np.pi / GRID)
    return np.cos(angle).astype(np.float32), np.sin(angle).astype(np.float32)


def y_factors():
    y = np.arange(256)[None, :]
    return *circle(16 * np.arange(32)[:, None] * y), *circle(np.arange(16)[:, None] * y)


def x_factors():
    kx = np.arange(256)[None, :]
    return *circle(32 * np.arange(16)[:, None] * kx), *circle(np.r_[0:32:2, 1:32:2][:, None] * kx)


def wave_rows():
    index = np.arange(GRID)
    back = (GRID - index) % GRID
    wave = (index - GRID * (index >= GRID // 2)) / (cell_nm * GRID)
    rows = [wave, wave * wave, np.exp(-RATE * wave * wave), wave[back]]
    return np.stack(rows).astype(np.float32)


def halves(value):
    high = value.astype(bf16)
    return high, (value - high.astype(f32)).astype(bf16)


def dot(a, b):
    return jnp.dot(a, b, preferred_element_type=f32)


def lane_index(shape):
    return lax.broadcasted_iota(jnp.int32, shape, len(shape) - 1)


def z_kernel(x_ref, high_ref, low_ref, out_ref, ext_ref):
    step = pl.program_id(0)
    core = step // 2
    x_high, x_low = halves(x_ref[...].reshape(256, GRID))
    w_high = high_ref[...]
    result = dot(x_high, w_high) + dot(x_low, w_high) + dot(x_high, low_ref[...])
    low_lanes = lane_index((32, 128)) < 64
    lane = lane_index((8, 128))
    for k in range(4):
        row = pl.multiple_of((step % 2) * 128 + k * 32, 32)
        even = result[k * 64 : k * 64 + 32]
        odd = result[k * 64 + 32 : k * 64 + 64]
        for t in range(4):
            e = even[:, t * 128 : t * 128 + 128]
            o = odd[:, t * 128 : t * 128 + 128]
            first = jnp.where(low_lanes, e, pltpu.roll(o, 64, 1))
            second = jnp.where(low_lanes, pltpu.roll(e, 64, 1), o)
            out_ref[core * 8 + t, pl.ds(row, 32), :] = first
            out_ref[core * 8 + 7 - t, pl.ds(row, 32), :] = second
        extra = jnp.zeros((8, 128), f32)
        for parity in range(2):
            for quarter in range(4):
                start = k * 64 + parity * 32 + quarter * 8
                piece = result[start : start + 8, 512:]
                here = (lane // 64 == parity) & (lane // 8 % 4 == quarter)
                extra = jnp.where(here, piece, extra)
        ext_ref[step * 4 + k] = extra

    @pl.when(step == 3)
    def _():
        for c in range(2):
            for h in range(8):
                packed = jnp.zeros((8, 128), f32)
                for x in range(8):
                    moved = pltpu.roll(ext_ref[c * 8 + x], (x - h) % 128, 1)
                    packed = jnp.where(lane % 8 == x, moved, packed)
                out_ref[c * 8 + (7 - h // 2 if h % 2 else h // 2), 256:EXT, :] = packed


def z_stage(block, tables):
    return pl.pallas_call(
        z_kernel,
        grid=(4,),
        in_specs=[
            pl.BlockSpec((8, 32, GRID), lambda i: (i, 0, 0)),
            pl.BlockSpec((GRID, 640), lambda i: (0, 0)),
            pl.BlockSpec((GRID, 640), lambda i: (0, 0)),
        ],
        out_specs=pl.BlockSpec((16, EXT, 128), lambda i: (0, 0, 0)),
        out_shape=jax.ShapeDtypeStruct((16, EXT, 128), f32),
        scratch_shapes=[pltpu.VMEM((16, 8, 128), f32)],
        name="z_stage",
        cost_estimate=pl.CostEstimate(flops=4 * 10**9, bytes_accessed=6 * 10**6, transcendentals=0),
    )(block, *tables)


def y_kernel(offsets, g_ref, pc_ref, ps_ref, oc_ref, os_ref, out_ref):
    rows = len(offsets)
    lane = lane_index((32, 128))
    real = lane // 32 % 2 == 0
    back = lane // 32 * 32 + (32 - lane % 32) % 32
    slot = lane % 32 == 0
    groups = [[o for o in offsets if o % 2 == parity] for parity in range(2)]
    pc = pc_ref[...]
    ps = ps_ref[...]
    tables = []
    for group in groups:
        cosines = [pc * oc_ref[o : o + 1, :] - ps * os_ref[o : o + 1, :] for o in group]
        sines = [ps * oc_ref[o : o + 1, :] + pc * os_ref[o : o + 1, :] for o in group]
        tables.append(halves(jnp.concatenate(cosines + sines, axis=0)))

    def products(low, high):
        results = []
        for (t_high, t_low), g in zip(tables, (low + high, low - high)):
            g_high, g_low = halves(g)
            results.append(dot(t_high, g_high) + dot(t_low, g_high) + dot(t_high, g_low))
        return results

    def pieces(results, columns):
        for parity, group in enumerate(groups):
            count = len(group) * 32
            for k, o in enumerate(group):
                p = results[parity][k * 32 : k * 32 + 32, columns]
                q = results[parity][count + k * 32 : count + k * 32 + 32, columns]
                turned = jnp.where(real, pltpu.roll(q, 96, 1), -pltpu.roll(q, 32, 1))
                other = p - turned
                yield offsets.index(o), p + turned, jnp.where(real, other, -other)

    def unpacked(start):
        parts = []
        for s in range(start, start + 8):
            packed = g_ref[s, 256:EXT, :]
            for quarter in range(4):
                parts.append(pltpu.roll(packed, 128 - 8 * quarter, 1) if quarter else packed)
        return jnp.concatenate(parts, axis=0)

    extra = {k: m for k, _, m in pieces(products(unpacked(0), unpacked(8)), slice(0, 128))}

    for pair in range(4):
        sides = []
        for start in (0, 8):
            columns = [
                g_ref[start : start + 8, x2 * 32 : x2 * 32 + 32, :].reshape(256, 128)
                for x2 in (2 * pair, 2 * pair + 1)
            ]
            sides.append(jnp.concatenate(columns, axis=1))
        results = products(*sides)
        for x2 in (2 * pair, 2 * pair + 1):
            first = x2 % 2 * 128
            for k, direct, mirror in pieces(results, slice(first, first + 128)):
                moved = pltpu.roll(extra[k], 128 - x2, 1) if x2 else extra[k]
                mirror = jnp.where(slot, moved, mirror)
                mirror = jnp.take_along_axis(mirror, back, axis=1)
                stride = 2 * rows * 8
                out_ref[pl.ds(k * 8 + x2, 32, stride=stride), :] = direct
                out_ref[pl.ds((rows + k) * 8 + x2, 32, stride=stride), :] = mirror


def x_table_rows(ac_ref, as_ref, bc_ref, bs_ref, high_ref, low_ref):
    for parity in range(2):
        bc = bc_ref[parity * 16 : parity * 16 + 16, :]
        bs = bs_ref[parity * 16 : parity * 16 + 16, :]
        for a in range(16):
            ac = ac_ref[a : a + 1, :]
            sa = as_ref[a : a + 1, :]
            full = jnp.concatenate([ac * bc - sa * bs, sa * bc + ac * bs], axis=1)
            high, low = halves(full)
            high_ref[parity, a * 16 : a * 16 + 16, :] = high
            low_ref[parity, a * 16 : a * 16 + 16, :] = low


def y_stage(blocks, offsets, with_tables):
    offsets = list(offsets)
    rows = len(offsets)

    def kernel(*refs):
        if with_tables:
            y_kernel(offsets, *refs[:5], refs[9])
            x_table_rows(*refs[5:9], *refs[10:])
        else:
            y_kernel(offsets, *refs)

    inputs = [blocks, *y_factors()]
    out_shape = [jax.ShapeDtypeStruct((64 * rows * 8, 128), f32)]
    if with_tables:
        inputs += x_factors()
        out_shape += [jax.ShapeDtypeStruct((2, 256, GRID), bf16)] * 2
    whole = pl.BlockSpec(memory_space=pltpu.VMEM)
    return pl.pallas_call(
        kernel,
        in_specs=[whole] * len(inputs),
        out_specs=[whole] * len(out_shape),
        out_shape=out_shape,
        name=f"y_stage_{rows}",
        cost_estimate=pl.CostEstimate(flops=4 * 10**9, bytes_accessed=6 * 10**6, transcendentals=0),
    )(*inputs)


def x_planes(high, g_ref, high_ref, low_ref, out_ref):
    turned = {}
    for o in range(STEP):
        for s in range(2):
            block = g_ref[:, s, o * 8 : o * 8 + 8, :].reshape(256, 128)
            turned[o, s] = jnp.transpose(block)
    half = STEP * 64
    real = []
    imag = []
    for parity in range(2):
        rows = [
            turned[o, s][parity * 64 + part * 32 : parity * 64 + part * 32 + 32]
            for part in range(2)
            for o in range(STEP)
            for s in range(2)
        ]
        a_high, a_low = halves(jnp.concatenate(rows, axis=0))
        w_high = high_ref[parity]
        result = dot(a_high, w_high) + dot(a_low, w_high) + dot(a_high, low_ref[parity])
        real.append(result[:half, :256] + result[half:, 256:])
        imag.append(result[half:, :256] - result[:half, 256:])
    full_real = jnp.concatenate([real[0] + real[1], real[0] - real[1]], axis=1)
    full_imag = jnp.concatenate([imag[0] + imag[1], imag[0] - imag[1]], axis=1)
    for o in range(STEP):
        for s in range(2):
            base = pl.multiple_of(32 * jnp.bitwise_xor(high, s), 32)
            start = o * 64 + s * 32
            out_ref[0, o, pl.ds(base, 32), :] = full_real[start : start + 32]
            out_ref[1, o, pl.ds(base, 32), :] = full_imag[start : start + 32]


def fold(value):
    return value.reshape(8, 8, GRID).sum(axis=0)


def x_kernel_a(side_ref, y_ref, g_ref, high_ref, low_ref, row_ref, col_ref, out_ref, sum_ref, acc_ref):
    step = pl.program_id(0)
    x_planes(side_ref[0], g_ref, high_ref, low_ref, out_ref)

    @pl.when(step == 0)
    def _():
        acc_ref[...] = jnp.zeros((7, 8, GRID), f32)

    mx = row_ref[0:1, :]
    mx_sq = row_ref[1:2, :]
    decay_x = row_ref[2:3, :]
    mx_back = row_ref[3:4, :]
    mod_x = row_ref[4:5, :]
    mod_x_back = row_ref[7:8, :]
    mz = col_ref[:, 0:1]
    mz_sq = col_ref[:, 1:2]
    decay_z = col_ref[:, 2:3]
    mz_back = col_ref[:, 3:4]
    mod_z = col_ref[:, 6:7]
    mod_z_back = col_ref[:, 9:10]
    for o in range(STEP):
        offset = step * STEP + o
        re = out_ref[0, o]
        im = out_ref[1, o]
        my = y_ref[0, offset]
        my_sq = y_ref[1, offset]
        decay_y = y_ref[2, offset]
        my_back = y_ref[3, offset]
        mod_y = y_ref[5, offset]
        paired = (offset >= 1) & (offset <= ROWS_B)
        mod_y_back = jnp.where(paired, y_ref[8, offset], 0.0)
        msq = mx_sq + (mz_sq + my_sq)
        anchor = msq == 0.0
        inverse = 1.0 / jnp.where(anchor, 1.0, msq)
        decay = decay_x * (decay_z * (decay_y * (1.0 / (math.pi * VOLUME))))
        base = decay * inverse * (re * re + im * im)
        base = jnp.where(anchor, 0.0, base)
        first = base * (mod_x * (mod_z * mod_y))
        second = base * (mod_x_back * (mod_z_back * mod_y_back))
        factor = (1.0 + RATE * msq) * inverse
        t1 = first * factor
        t2 = second * factor
        s1 = fold(t1)
        s2 = fold(t2)
        both = s1 + s2
        z1 = fold(t1 * mz)
        z2 = fold(t2 * mz_back)
        acc_ref[0] += fold(first + second)
        acc_ref[1] += both * mx_sq
        acc_ref[2] += both * my_sq
        acc_ref[3] += fold((t1 + t2) * mz_sq)
        acc_ref[4] += s1 * (mx * my) + s2 * (mx_back * my_back)
        acc_ref[5] += z1 * mx + z2 * mx_back
        acc_ref[6] += z1 * my + z2 * my_back

    @pl.when(step == pl.num_programs(0) - 1)
    def _():
        total = acc_ref[...]
        total = total[:, :, :128] + total[:, :, 128:256] + total[:, :, 256:384] + total[:, :, 384:]
        sum_ref[0:7, :] = total.sum(axis=1)
        sum_ref[7:8, :] = jnp.zeros((1, 128), f32)


def x_kernel_b(side_ref, g_ref, high_ref, low_ref, whole_ref, out_ref):
    del whole_ref
    x_planes(side_ref[0], g_ref, high_ref, low_ref, out_ref)


def x_specs():
    return [
        pl.BlockSpec((32, 2, STEP * 8, 128), lambda i: (0, 0, i, 0)),
        pl.BlockSpec((2, 256, GRID), lambda i: (0, 0, 0)),
        pl.BlockSpec((2, 256, GRID), lambda i: (0, 0, 0)),
    ]


OUT_SHAPE = jax.ShapeDtypeStruct((2, 16, 64, GRID), f32)


def x_stage_a(side, y_numbers, blocks, tables, row_numbers, col_numbers):
    smem = pl.BlockSpec(memory_space=pltpu.SMEM)
    return pl.pallas_call(
        x_kernel_a,
        grid=(ROWS_A // STEP,),
        in_specs=[
            smem,
            smem,
            *x_specs(),
            pl.BlockSpec((10, GRID), lambda i: (0, 0)),
            pl.BlockSpec((64, 10), lambda i: (0, 0)),
        ],
        out_specs=[
            pl.BlockSpec((2, STEP, 64, GRID), lambda i: (0, i, 0, 0)),
            pl.BlockSpec((8, 128), lambda i: (0, 0)),
        ],
        out_shape=[OUT_SHAPE, jax.ShapeDtypeStruct((8, 128), f32)],
        scratch_shapes=[pltpu.VMEM((7, 8, GRID), f32)],
        name="x_stage_a",
        cost_estimate=pl.CostEstimate(flops=4 * 10**9, bytes_accessed=6 * 10**6, transcendentals=0),
    )(side, y_numbers, blocks, *tables, row_numbers, col_numbers)


def x_stage_b(side, blocks, tables, whole):
    smem = pl.BlockSpec(memory_space=pltpu.SMEM)
    return pl.pallas_call(
        x_kernel_b,
        grid=(ROWS_B // STEP,),
        in_specs=[smem, *x_specs(), pl.BlockSpec(memory_space=pl.ANY)],
        out_specs=pl.BlockSpec((2, STEP, 64, GRID), lambda i: (0, ROWS_A // STEP + i, 0, 0)),
        out_shape=OUT_SHAPE,
        input_output_aliases={4: 0},
        name="x_stage_b",
        cost_estimate=pl.CostEstimate(flops=4 * 10**9, bytes_accessed=6 * 10**6, transcendentals=0),
    )(side, blocks, *tables, whole)


def pair_groups():
    ids = np.arange(256).reshape(32, 8)
    return [
        np.stack([ids[:, q], ids[:, 7 - q]], axis=1).reshape(-1).tolist() for q in range(4)
    ]


def exchange(blocks, rows):
    blocks = blocks.reshape(64, rows * 8, 128)
    blocks = lax.all_to_all(
        blocks, ALL, split_axis=0, concat_axis=0, tiled=True, axis_index_groups=pair_groups()
    )
    return blocks.reshape(32, 2, rows * 8, 128)


def all_sum(value):
    for axis in (("px_2",), ("px_0",), ("py_1",), ("px_1", "py_0")):
        size = lax.axis_size(axis)
        parts = [value]
        for k in range(1, size):
            parts.append(lax.ppermute(value, axis, [(s, s ^ k) for s in range(size)]))
        while len(parts) > 1:
            parts = [a + b for a, b in zip(parts[::2], parts[1::2])]
        value = parts[0]
    return value


def body(charges_old, spline_moduli):
    row_position = lax.axis_index(PX)
    col_position = lax.axis_index(PY)
    side = (col_position >= 4).astype(jnp.int32)
    planes = z_stage(charges_old[0, 0], z_table())
    planes = lax.all_to_all(planes, FIRST, split_axis=0, concat_axis=0, tiled=True)

    backward = jnp.roll(jnp.flip(spline_moduli, axis=1), 1, axis=1)
    numbers = jnp.concatenate([jnp.asarray(wave_rows()), spline_moduli, backward])
    col_numbers = lax.dynamic_slice_in_dim(numbers, col_position * 64, 64, axis=1).T
    y_numbers = lax.dynamic_slice_in_dim(numbers, row_position * 16, 16, axis=1)

    (part_a,) = y_stage(planes, range(ROWS_A), False)
    part_a = exchange(part_a, ROWS_A)
    planes, numbers, col_numbers, y_numbers = lax.optimization_barrier(
        (planes, numbers, col_numbers, y_numbers)
    )
    part_b, *tables_x = y_stage(planes, range(ROWS_A, 16), True)
    part_b = exchange(part_b, ROWS_B)

    whole, sums = x_stage_a(side.reshape(1), y_numbers, part_a, tables_x, numbers, col_numbers)
    sums = all_sum(sums).sum(axis=1)
    structure = x_stage_b(side.reshape(1), part_b, tables_x, whole)
    energy = 0.5 * sums[0]
    virial = energy * jnp.array([1.0, 1.0, 1.0, 0.0, 0.0, 0.0], dtype=f32) - sums[1:7]
    return structure, energy, virial


def solution(mesh):
    torus = Mesh(mesh.devices.reshape(4, 4, 2, 2, 4), ALL)
    return jax.shard_map(
        body,
        mesh=torus,
        in_specs=(P(PX, PY, None, None, None), P()),
        out_specs=(P(None, PX, PY, None), P(), P()),
        check_vma=False,
    )
```

```python
import math

import jax
import jax.numpy as jnp
import numpy as np
from jax import lax
from jax.experimental import pallas as pl
from jax.experimental.pallas import tpu as pltpu
from jax.sharding import Mesh
from jax.sharding import PartitionSpec as P

PX = ("px_0", "px_1", "px_2")
PY = ("py_0", "py_1")
ALL = ("px_0", "px_1", "px_2", "py_0", "py_1")
FIRST = ("px_2", "py_0", "py_1")

GRID = 512
beta_nm = 3.12
cell_nm = 0.1
RATE = math.pi**2 / beta_nm**2
VOLUME = (cell_nm * GRID) ** 3
ROWS_A = 10
ROWS_B = 6
STEP = 2
EXT = 264
f32 = jnp.float32
bf16 = jnp.bfloat16


def split_table(table):
    high = table.astype(bf16)
    low = (table - high.astype(np.float64)).astype(bf16)
    return high, low


def z_table():
    z = np.arange(GRID)[:, None]
    column = np.arange(GRID)[None, :]
    kz = column // 64 * 32 + column % 32
    part = column // 32 % 2
    lane = np.arange(128)[None, :]
    kz = np.concatenate([kz, (lane % 8 + 1) * 32], axis=1)
    part = np.concatenate([part, lane // 32 % 2], axis=1)
    angle = z * kz % GRID * (2.0 * np.pi / GRID)
    return split_table(np.where(part == 0, np.cos(angle), -np.sin(angle)))


def circle(turns):
    angle = turns % GRID * (2.0 * np.pi / GRID)
    return np.cos(angle).astype(np.float32), np.sin(angle).astype(np.float32)


def y_factors():
    y = np.arange(256)[None, :]
    return *circle(16 * np.arange(32)[:, None] * y), *circle(np.arange(16)[:, None] * y)


def x_factors():
    kx = np.arange(256)[None, :]
    return *circle(32 * np.arange(16)[:, None] * kx), *circle(np.r_[0:32:2, 1:32:2][:, None] * kx)


def wave_rows():
    index = np.arange(GRID)
    back = (GRID - index) % GRID
    wave = (index - GRID * (index >= GRID // 2)) / (cell_nm * GRID)
    rows = [wave, wave * wave, np.exp(-RATE * wave * wave), wave[back]]
    return np.stack(rows).astype(np.float32)


def halves(value):
    high = value.astype(bf16)
    return high, (value - high.astype(f32)).astype(bf16)


def dot(a, b):
    return jnp.dot(a, b, preferred_element_type=f32)


def lane_index(shape):
    return lax.broadcasted_iota(jnp.int32, shape, len(shape) - 1)


def z_kernel(x_ref, high_ref, low_ref, out_ref, ext_ref):
    step = pl.program_id(0)
    core = step // 2
    x_high, x_low = halves(x_ref[...].reshape(256, GRID))
    w_high = high_ref[...]
    result = dot(x_high, w_high) + dot(x_low, w_high) + dot(x_high, low_ref[...])
    low_lanes = lane_index((32, 128)) < 64
    lane = lane_index((8, 128))
    for k in range(4):
        row = pl.multiple_of((step % 2) * 128 + k * 32, 32)
        even = result[k * 64 : k * 64 + 32]
        odd = result[k * 64 + 32 : k * 64 + 64]
        for t in range(4):
            e = even[:, t * 128 : t * 128 + 128]
            o = odd[:, t * 128 : t * 128 + 128]
            first = jnp.where(low_lanes, e, pltpu.roll(o, 64, 1))
            second = jnp.where(low_lanes, pltpu.roll(e, 64, 1), o)
            out_ref[core * 8 + t, pl.ds(row, 32), :] = first
            out_ref[core * 8 + 7 - t, pl.ds(row, 32), :] = second
        extra = jnp.zeros((8, 128), f32)
        for parity in range(2):
            for quarter in range(4):
                start = k * 64 + parity * 32 + quarter * 8
                piece = result[start : start + 8, 512:]
                here = (lane // 64 == parity) & (lane // 8 % 4 == quarter)
                extra = jnp.where(here, piece, extra)
        ext_ref[step * 4 + k] = extra

    @pl.when(step == 3)
    def _():
        for c in range(2):
            for h in range(8):
                packed = jnp.zeros((8, 128), f32)
                for x in range(8):
                    moved = pltpu.roll(ext_ref[c * 8 + x], (x - h) % 128, 1)
                    packed = jnp.where(lane % 8 == x, moved, packed)
                out_ref[c * 8 + (7 - h // 2 if h % 2 else h // 2), 256:EXT, :] = packed


def z_stage(block, tables):
    return pl.pallas_call(
        z_kernel,
        grid=(4,),
        in_specs=[
            pl.BlockSpec((8, 32, GRID), lambda i: (i, 0, 0)),
            pl.BlockSpec((GRID, 640), lambda i: (0, 0)),
            pl.BlockSpec((GRID, 640), lambda i: (0, 0)),
        ],
        out_specs=pl.BlockSpec((16, EXT, 128), lambda i: (0, 0, 0)),
        out_shape=pltpu.MemorySpace.VMEM((16, EXT, 128), f32),
        scratch_shapes=[pltpu.VMEM((16, 8, 128), f32)],
        name="z_stage",
        cost_estimate=pl.CostEstimate(flops=4 * 10**9, bytes_accessed=6 * 10**6, transcendentals=0),
    )(block, *tables)


def y_rows(offsets, parts, g_ref, factor_refs, stage_ref, ready, deliver):
    pc_ref, ps_ref, oc_ref, os_ref = factor_refs
    rows = len(offsets)
    size = 32 // parts
    pitch = rows * 64 + 8
    lane = lane_index((size, 128))
    real = lane // 32 % 2 == 0
    back = lane // 32 * 32 + (32 - lane % 32) % 32
    slot = lane % 32 == 0
    groups = [[o for o in offsets if o % 2 == parity] for parity in range(2)]

    def tables_of(part):
        pc = pc_ref[part * size : part * size + size, :]
        ps = ps_ref[part * size : part * size + size, :]
        tables = []
        for group in groups:
            cosines = [pc * oc_ref[o : o + 1, :] - ps * os_ref[o : o + 1, :] for o in group]
            sines = [ps * oc_ref[o : o + 1, :] + pc * os_ref[o : o + 1, :] for o in group]
            tables.append(halves(jnp.concatenate(cosines + sines, axis=0)))
        return tables

    def products(tables, low, high):
        results = []
        for (t_high, t_low), g in zip(tables, (low + high, low - high)):
            g_high, g_low = halves(g)
            results.append(dot(t_high, g_high) + dot(t_low, g_high) + dot(t_high, g_low))
        return results

    def pieces(results, columns):
        for parity, group in enumerate(groups):
            count = len(group) * size
            for k, o in enumerate(group):
                p = results[parity][k * size : k * size + size, columns]
                q = results[parity][count + k * size : count + k * size + size, columns]
                turned = jnp.where(real, pltpu.roll(q, 96, 1), -pltpu.roll(q, 32, 1))
                other = p - turned
                yield offsets.index(o), p + turned, jnp.where(real, other, -other)

    def unpacked(start):
        blocks = []
        for s in range(start, start + 8):
            packed = g_ref[s, 256:EXT, :]
            for quarter in range(4):
                blocks.append(pltpu.roll(packed, 128 - 8 * quarter, 1) if quarter else packed)
        return jnp.concatenate(blocks, axis=0)

    for part in range(parts):
        tables = tables_of(part)
        ready(4, part)
        results = products(tables, unpacked(0), unpacked(8))
        extra = {k: m for k, _, m in pieces(results, slice(0, 128))}
        for pair in range(4):
            ready(pair, part)
            sides = []
            for start in (0, 8):
                columns = [
                    g_ref[start : start + 8, x2 * 32 : x2 * 32 + 32, :].reshape(256, 128)
                    for x2 in (2 * pair, 2 * pair + 1)
                ]
                sides.append(jnp.concatenate(columns, axis=1))
            results = products(tables, *sides)
            for x2 in (2 * pair, 2 * pair + 1):
                first = x2 % 2 * 128
                for k, direct, mirror in pieces(results, slice(first, first + 128)):
                    moved = pltpu.roll(extra[k], 128 - x2, 1) if x2 else extra[k]
                    mirror = jnp.where(slot, moved, mirror)
                    mirror = jnp.take_along_axis(mirror, back, axis=1)
                    at = x2 * pitch + k * 32 + part * size
                    stage_ref[at : at + size, :] = direct
                    stage_ref[at + rows * 32 : at + rows * 32 + size, :] = mirror
        deliver(part)


def y_kernel_a(offsets, g_ref, pc_ref, ps_ref, oc_ref, os_ref, target_ref, copy_ref, out_ref, stage_ref, copy_sem, out_sems):
    rows = len(offsets)
    pitch = rows * 64 + 8
    copy = pltpu.make_async_copy(g_ref, copy_ref, copy_sem)
    copy.start()

    def flush(part):
        window = pl.ds(part * 32, 32)
        return pltpu.make_async_copy(out_ref.at[window], target_ref.at[window], out_sems.at[part])

    def gather(p, carry):
        for pair in range(2):
            for k in range(rows):
                first = (pair * rows + k) * 32 + p
                block = stage_ref[pl.ds(first, 8, stride=pitch), :]
                out_ref[2 * p + pair, k * 8 : k * 8 + 8, :] = block
        return carry

    def deliver(part):
        lax.fori_loop(part * 16, part * 16 + 16, gather, 0)
        flush(part).start()

    factors = (pc_ref, ps_ref, oc_ref, os_ref)
    y_rows(offsets, 2, g_ref, factors, stage_ref, lambda *_: None, deliver)
    copy.wait()
    flush(0).wait()
    flush(1).wait()


def y_kernel_b(offsets, core_ref, g_ref, pc_ref, ps_ref, oc_ref, os_ref, keep_ref, send_ref, stage_ref):
    rows = len(offsets)
    pitch = rows * 64 + 8
    core = core_ref[0]

    def gather(p, carry):
        for out_ref, side in ((keep_ref, core), (send_ref, 1 - core)):
            for pair in range(2):
                for k in range(rows):
                    first = (pair * rows + k) * 32 + 2 * p + side
                    block = stage_ref[pl.ds(first, 8, stride=pitch), :]
                    out_ref[2 * p + pair, k * 8 : k * 8 + 8, :] = block
        return carry

    def deliver(part):
        lax.fori_loop(0, 16, gather, 0)

    factors = (pc_ref, ps_ref, oc_ref, os_ref)
    y_rows(offsets, 1, g_ref, factors, stage_ref, lambda *_: None, deliver)


WHOLE = pl.BlockSpec(memory_space=pltpu.VMEM)
SMALL = pltpu.CompilerParams(vmem_limit_bytes=24 * 2**20)


def y_stage_a(blocks):
    rows = ROWS_A

    def kernel(*refs):
        y_kernel_a(list(range(ROWS_A)), *refs)

    hbm = pl.BlockSpec(memory_space=pltpu.HBM)
    return pl.pallas_call(
        kernel,
        in_specs=[WHOLE] * 5,
        out_specs=[hbm, hbm],
        out_shape=[
            pltpu.MemorySpace.HBM((64, rows * 8, 128), f32),
            pltpu.MemorySpace.HBM((16, EXT, 128), f32),
        ],
        scratch_shapes=[
            pltpu.VMEM((64, rows * 8, 128), f32),
            pltpu.VMEM((8 * (rows * 64 + 8), 128), f32),
            pltpu.SemaphoreType.DMA,
            pltpu.SemaphoreType.DMA((2,)),
        ],
        compiler_params=SMALL,
        name="y_stage_a",
        cost_estimate=pl.CostEstimate(flops=4 * 10**9, bytes_accessed=6 * 10**6, transcendentals=0),
    )(blocks, *y_factors())


def y_stage_b(core, blocks):
    rows = ROWS_B

    def kernel(*refs):
        y_kernel_b(list(range(ROWS_A, 16)), *refs)

    return pl.pallas_call(
        kernel,
        in_specs=[pl.BlockSpec(memory_space=pltpu.SMEM)] + [WHOLE] * 5,
        out_specs=[WHOLE, WHOLE],
        out_shape=[jax.ShapeDtypeStruct((32, rows * 8, 128), f32)] * 2,
        scratch_shapes=[pltpu.VMEM((8 * (rows * 64 + 8), 128), f32)],
        name="y_stage_b",
        cost_estimate=pl.CostEstimate(flops=4 * 10**9, bytes_accessed=6 * 10**6, transcendentals=0),
    )(core, blocks, *y_factors())


def x_tables(ac_ref, as_ref, bc_ref, bs_ref, high_ref, low_ref):
    for parity in range(2):
        bc = bc_ref[parity * 16 : parity * 16 + 16, :]
        bs = bs_ref[parity * 16 : parity * 16 + 16, :]
        for a in range(16):
            ac = ac_ref[a : a + 1, :]
            sa = as_ref[a : a + 1, :]
            full = jnp.concatenate([ac * bc - sa * bs, sa * bc + ac * bs], axis=1)
            high, low = halves(full)
            high_ref[parity, a * 16 : a * 16 + 16, :] = high
            low_ref[parity, a * 16 : a * 16 + 16, :] = low


def y_stage(blocks, offsets):
    offsets = list(offsets)
    rows = len(offsets)

    def kernel(*refs):
        y_kernel(offsets, *refs)

    whole = pl.BlockSpec(memory_space=pltpu.VMEM)
    hbm = pl.BlockSpec(memory_space=pltpu.HBM)
    return pl.pallas_call(
        kernel,
        in_specs=[hbm] + [whole] * 4,
        out_specs=hbm,
        out_shape=jax.ShapeDtypeStruct((64, rows * 8, 128), f32),
        scratch_shapes=[
            pltpu.VMEM((16, EXT, 128), f32),
            pltpu.VMEM((64, rows * 8, 128), f32),
            pltpu.VMEM((8 * (rows * 64 + 8), 128), f32),
            pltpu.SemaphoreType.DMA((5,)),
            pltpu.SemaphoreType.DMA((4,)),
        ],
        name=f"y_stage_{rows}",
        cost_estimate=pl.CostEstimate(flops=4 * 10**9, bytes_accessed=6 * 10**6, transcendentals=0),
    )(blocks, *y_factors())


def x_planes(high, g_ref, high_ref, low_ref, out_ref):
    turned = {}
    for o in range(STEP):
        for s in range(2):
            if len(g_ref.shape) == 5:
                block = g_ref[:, s, :, o * 8 : o * 8 + 8, :]
            else:
                block = g_ref[:, s, o * 8 : o * 8 + 8, :]
            block = block.reshape(256, 128)
            turned[o, s] = jnp.transpose(block)
    half = STEP * 64
    real = []
    imag = []
    for parity in range(2):
        rows = [
            turned[o, s][parity * 64 + part * 32 : parity * 64 + part * 32 + 32]
            for part in range(2)
            for o in range(STEP)
            for s in range(2)
        ]
        a_high, a_low = halves(jnp.concatenate(rows, axis=0))
        w_high = high_ref[parity]
        result = dot(a_high, w_high) + dot(a_low, w_high) + dot(a_high, low_ref[parity])
        real.append(result[:half, :256] + result[half:, 256:])
        imag.append(result[half:, :256] - result[:half, 256:])
    full_real = jnp.concatenate([real[0] + real[1], real[0] - real[1]], axis=1)
    full_imag = jnp.concatenate([imag[0] + imag[1], imag[0] - imag[1]], axis=1)
    for o in range(STEP):
        for s in range(2):
            base = pl.multiple_of(32 * jnp.bitwise_xor(high, s), 32)
            start = o * 64 + s * 32
            out_ref[0, o, pl.ds(base, 32), :] = full_real[start : start + 32]
            out_ref[1, o, pl.ds(base, 32), :] = full_imag[start : start + 32]


def fold(value):
    return value.reshape(8, 8, GRID).sum(axis=0)


def x_kernel_a(side_ref, y_ref, g_ref, ac_ref, as_ref, bc_ref, bs_ref, row_ref, col_ref, out_ref, sum_ref, acc_ref, high_ref, low_ref):
    step = pl.program_id(0)

    @pl.when(step == 0)
    def _():
        x_tables(ac_ref, as_ref, bc_ref, bs_ref, high_ref, low_ref)

    x_planes(side_ref[0], g_ref, high_ref, low_ref, out_ref)

    @pl.when(step == 0)
    def _():
        acc_ref[...] = jnp.zeros((7, 8, GRID), f32)

    mx = row_ref[0:1, :]
    mx_sq = row_ref[1:2, :]
    decay_x = row_ref[2:3, :]
    mx_back = row_ref[3:4, :]
    mod_x = row_ref[4:5, :]
    mod_x_back = row_ref[7:8, :]
    mz = col_ref[:, 0:1]
    mz_sq = col_ref[:, 1:2]
    decay_z = col_ref[:, 2:3]
    mz_back = col_ref[:, 3:4]
    mod_z = col_ref[:, 6:7]
    mod_z_back = col_ref[:, 9:10]
    for o in range(STEP):
        offset = step * STEP + o
        re = out_ref[0, o]
        im = out_ref[1, o]
        my = y_ref[0, offset]
        my_sq = y_ref[1, offset]
        decay_y = y_ref[2, offset]
        my_back = y_ref[3, offset]
        mod_y = y_ref[5, offset]
        paired = (offset >= 1) & (offset <= ROWS_B)
        mod_y_back = jnp.where(paired, y_ref[8, offset], 0.0)
        msq = mx_sq + (mz_sq + my_sq)
        anchor = msq == 0.0
        inverse = 1.0 / jnp.where(anchor, 1.0, msq)
        decay = decay_x * (decay_z * (decay_y * (1.0 / (math.pi * VOLUME))))
        base = decay * inverse * (re * re + im * im)
        base = jnp.where(anchor, 0.0, base)
        first = base * (mod_x * (mod_z * mod_y))
        second = base * (mod_x_back * (mod_z_back * mod_y_back))
        factor = (1.0 + RATE * msq) * inverse
        t1 = first * factor
        t2 = second * factor
        s1 = fold(t1)
        s2 = fold(t2)
        both = s1 + s2
        z1 = fold(t1 * mz)
        z2 = fold(t2 * mz_back)
        acc_ref[0] += fold(first + second)
        acc_ref[1] += both * mx_sq
        acc_ref[2] += both * my_sq
        acc_ref[3] += fold((t1 + t2) * mz_sq)
        acc_ref[4] += s1 * (mx * my) + s2 * (mx_back * my_back)
        acc_ref[5] += z1 * mx + z2 * mx_back
        acc_ref[6] += z1 * my + z2 * my_back

    @pl.when(step == pl.num_programs(0) - 1)
    def _():
        total = acc_ref[...]
        total = total[:, :, :128] + total[:, :, 128:256] + total[:, :, 256:384] + total[:, :, 384:]
        sum_ref[0:7, :] = total.sum(axis=1)
        sum_ref[7:8, :] = jnp.zeros((1, 128), f32)


def x_kernel_b(side_ref, g_ref, ac_ref, as_ref, bc_ref, bs_ref, whole_ref, out_ref, high_ref, low_ref):
    del whole_ref

    @pl.when(pl.program_id(0) == 0)
    def _():
        x_tables(ac_ref, as_ref, bc_ref, bs_ref, high_ref, low_ref)

    x_planes(side_ref[0], g_ref, high_ref, low_ref, out_ref)


FACTORS = [pl.BlockSpec((rows, 256), lambda i: (0, 0)) for rows in (16, 16, 32, 32)]
TABLES = [pltpu.VMEM((2, 256, GRID), bf16)] * 2
OUT_SHAPE = jax.ShapeDtypeStruct((2, 16, 64, GRID), f32)


def x_stage_a(side, y_numbers, blocks, row_numbers, col_numbers):
    smem = pl.BlockSpec(memory_space=pltpu.SMEM)
    return pl.pallas_call(
        x_kernel_a,
        grid=(ROWS_A // STEP,),
        in_specs=[
            smem,
            smem,
            pl.BlockSpec((32, 2, STEP * 8, 128), lambda i: (0, 0, i, 0)),
            *FACTORS,
            pl.BlockSpec((10, GRID), lambda i: (0, 0)),
            pl.BlockSpec((64, 10), lambda i: (0, 0)),
        ],
        out_specs=[
            pl.BlockSpec((2, STEP, 64, GRID), lambda i: (0, i, 0, 0)),
            pl.BlockSpec((8, 128), lambda i: (0, 0)),
        ],
        out_shape=[OUT_SHAPE, jax.ShapeDtypeStruct((8, 128), f32)],
        scratch_shapes=[pltpu.VMEM((7, 8, GRID), f32), *TABLES],
        compiler_params=pltpu.CompilerParams(vmem_limit_bytes=24 * 2**20),
        name="x_stage_a",
        cost_estimate=pl.CostEstimate(flops=4 * 10**9, bytes_accessed=6 * 10**6, transcendentals=0),
    )(side, y_numbers, blocks, *x_factors(), row_numbers, col_numbers)


def x_stage_b(side, blocks, whole):
    smem = pl.BlockSpec(memory_space=pltpu.SMEM)
    return pl.pallas_call(
        x_kernel_b,
        grid=(ROWS_B // STEP,),
        in_specs=[
            smem,
            pl.BlockSpec((16, 2, 2, STEP * 8, 128), lambda i: (0, 0, 0, i, 0)),
            *FACTORS,
            pl.BlockSpec(memory_space=pl.ANY),
        ],
        out_specs=pl.BlockSpec((2, STEP, 64, GRID), lambda i: (0, ROWS_A // STEP + i, 0, 0)),
        out_shape=OUT_SHAPE,
        scratch_shapes=TABLES,
        input_output_aliases={6: 0},
        compiler_params=pltpu.CompilerParams(vmem_limit_bytes=24 * 2**20),
        name="x_stage_b",
        cost_estimate=pl.CostEstimate(flops=4 * 10**9, bytes_accessed=6 * 10**6, transcendentals=0),
    )(side, blocks, *x_factors(), whole)


def pair_groups(split_cores):
    ids = np.arange(256).reshape(16, 2, 8)
    groups = []
    for q in range(4):
        members = np.stack([ids[:, :, q], ids[:, :, 7 - q]], axis=2)
        if split_cores:
            groups += [members[:, core].reshape(-1).tolist() for core in range(2)]
        else:
            groups.append(members.reshape(-1).tolist())
    return groups


def exchange(blocks, split_cores):
    return lax.all_to_all(
        blocks, ALL, split_axis=0, concat_axis=0, tiled=True, axis_index_groups=pair_groups(split_cores)
    )


def all_sum(value):
    for axis in (("px_2",), ("px_0",), ("py_1",), ("px_1",), ("py_0",)):
        size = lax.axis_size(axis)
        parts = [value]
        for k in range(1, size):
            parts.append(lax.ppermute(value, axis, [(s, s ^ k) for s in range(size)]))
        while len(parts) > 1:
            parts = [a + b for a, b in zip(parts[::2], parts[1::2])]
        value = parts[0]
    return value


def body(charges_old, spline_moduli):
    row_position = lax.axis_index(PX)
    col_position = lax.axis_index(PY)
    side = (col_position >= 4).astype(jnp.int32)
    planes = z_stage(charges_old[0, 0], z_table())
    planes = lax.all_to_all(planes, FIRST, split_axis=0, concat_axis=0, tiled=True)

    backward = jnp.roll(jnp.flip(spline_moduli, axis=1), 1, axis=1)
    numbers = jnp.concatenate([jnp.asarray(wave_rows()), spline_moduli, backward])
    col_numbers = lax.dynamic_slice_in_dim(numbers, col_position * 64, 64, axis=1).T
    y_numbers = lax.dynamic_slice_in_dim(numbers, row_position * 16, 16, axis=1)

    part_a, planes = y_stage_a(planes)
    part_a = exchange(part_a, False).reshape(32, 2, ROWS_A * 8, 128)
    planes, numbers, col_numbers, y_numbers = lax.optimization_barrier(
        (planes, numbers, col_numbers, y_numbers)
    )
    core = lax.axis_index("px_2")
    keep, send = y_stage_b(core.reshape(1), planes)
    received = lax.ppermute(send, "px_2", [(0, 1), (1, 0)])
    lower = core == 0
    halves_of_x = [jnp.where(lower, keep, received), jnp.where(lower, received, keep)]
    part_b = exchange(jnp.stack(halves_of_x, axis=1), True).reshape(16, 2, 2, ROWS_B * 8, 128)

    whole, sums = x_stage_a(side.reshape(1), y_numbers, part_a, numbers, col_numbers)
    sums = all_sum(sums).sum(axis=1)
    structure = x_stage_b(side.reshape(1), part_b, whole)
    energy = 0.5 * sums[0]
    virial = energy * jnp.array([1.0, 1.0, 1.0, 0.0, 0.0, 0.0], dtype=f32) - sums[1:7]
    return structure, energy, virial


def solution(mesh):
    torus = Mesh(mesh.devices.reshape(4, 4, 2, 2, 4), ALL)
    return jax.shard_map(
        body,
        mesh=torus,
        in_specs=(P(PX, PY, None, None, None), P()),
        out_specs=(P(None, PX, PY, None), P(), P()),
        check_vma=False,
    )
```

```python
import math

import jax
import jax.numpy as jnp
import numpy as np
from jax import lax
from jax.experimental import pallas as pl
from jax.experimental.pallas import tpu as pltpu
from jax.sharding import Mesh
from jax.sharding import PartitionSpec as P

PX = ("px_0", "px_1", "px_2")
PY = ("py_0", "py_1")
ALL = ("px_0", "px_1", "px_2", "py_0", "py_1")
FIRST = ("px_2", "py_0", "py_1")

GRID = 512
beta_nm = 3.12
cell_nm = 0.1
RATE = math.pi**2 / beta_nm**2
VOLUME = (cell_nm * GRID) ** 3
ROWS_A = 10
ROWS_B = 6
STEP = 2
EXT = 264
f32 = jnp.float32
bf16 = jnp.bfloat16


def split_table(table):
    high = table.astype(bf16)
    low = (table - high.astype(np.float64)).astype(bf16)
    return high, low


def z_table():
    z = np.arange(GRID)[:, None]
    column = np.arange(GRID)[None, :]
    kz = column // 64 * 32 + column % 32
    part = column // 32 % 2
    lane = np.arange(128)[None, :]
    kz = np.concatenate([kz, (lane % 8 + 1) * 32], axis=1)
    part = np.concatenate([part, lane // 32 % 2], axis=1)
    angle = z * kz % GRID * (2.0 * np.pi / GRID)
    return split_table(np.where(part == 0, np.cos(angle), -np.sin(angle)))


def circle(turns):
    angle = turns % GRID * (2.0 * np.pi / GRID)
    return np.cos(angle).astype(np.float32), np.sin(angle).astype(np.float32)


def y_factors():
    y = np.arange(256)[None, :]
    return *circle(16 * np.arange(32)[:, None] * y), *circle(np.arange(16)[:, None] * y)


def x_factors():
    kx = np.arange(256)[None, :]
    return *circle(32 * np.arange(16)[:, None] * kx), *circle(np.r_[0:32:2, 1:32:2][:, None] * kx)


def wave_rows():
    index = np.arange(GRID)
    back = (GRID - index) % GRID
    wave = (index - GRID * (index >= GRID // 2)) / (cell_nm * GRID)
    rows = [wave, wave * wave, np.exp(-RATE * wave * wave), wave[back]]
    return np.stack(rows).astype(np.float32)


def halves(value):
    high = value.astype(bf16)
    return high, (value - high.astype(f32)).astype(bf16)


def dot(a, b):
    return jnp.dot(a, b, preferred_element_type=f32)


def lane_index(shape):
    return lax.broadcasted_iota(jnp.int32, shape, len(shape) - 1)


def z_kernel(x_ref, high_ref, low_ref, out_ref, ext_ref):
    step = pl.program_id(0)
    core = step // 1
    x_high, x_low = halves(x_ref[...].reshape(512, GRID))
    w_high = high_ref[...]
    result = dot(x_high, w_high) + dot(x_low, w_high) + dot(x_high, low_ref[...])
    low_lanes = lane_index((32, 128)) < 64
    lane = lane_index((8, 128))
    for k in range(8):
        row = pl.multiple_of((step % 1) * 256 + k * 32, 32)
        even = result[k * 64 : k * 64 + 32]
        odd = result[k * 64 + 32 : k * 64 + 64]
        for t in range(4):
            e = even[:, t * 128 : t * 128 + 128]
            o = odd[:, t * 128 : t * 128 + 128]
            first = jnp.where(low_lanes, e, pltpu.roll(o, 64, 1))
            second = jnp.where(low_lanes, pltpu.roll(e, 64, 1), o)
            out_ref[core * 8 + t, pl.ds(row, 32), :] = first
            out_ref[core * 8 + 7 - t, pl.ds(row, 32), :] = second
        extra = jnp.zeros((8, 128), f32)
        for parity in range(2):
            for quarter in range(4):
                start = k * 64 + parity * 32 + quarter * 8
                piece = result[start : start + 8, 512:]
                here = (lane // 64 == parity) & (lane // 8 % 4 == quarter)
                extra = jnp.where(here, piece, extra)
        ext_ref[step * 8 + k] = extra

    @pl.when(step == 1)
    def _():
        for c in range(2):
            for h in range(8):
                packed = jnp.zeros((8, 128), f32)
                for x in range(8):
                    moved = pltpu.roll(ext_ref[c * 8 + x], (x - h) % 128, 1)
                    packed = jnp.where(lane % 8 == x, moved, packed)
                out_ref[c * 8 + (7 - h // 2 if h % 2 else h // 2), 256:EXT, :] = packed


def z_stage(block, tables):
    return pl.pallas_call(
        z_kernel,
        grid=(2,),
        in_specs=[
            pl.BlockSpec((16, 32, GRID), lambda i: (i, 0, 0)),
            pl.BlockSpec((GRID, 640), lambda i: (0, 0)),
            pl.BlockSpec((GRID, 640), lambda i: (0, 0)),
        ],
        out_specs=pl.BlockSpec((16, EXT, 128), lambda i: (0, 0, 0)),
        out_shape=pltpu.MemorySpace.VMEM((16, EXT, 128), f32),
        scratch_shapes=[pltpu.VMEM((16, 8, 128), f32)],
        name="z_stage",
        cost_estimate=pl.CostEstimate(flops=4 * 10**9, bytes_accessed=6 * 10**6, transcendentals=0),
    )(block, *tables)


def y_rows(offsets, parts, g_ref, factor_refs, stage_ref, ready, deliver):
    pc_ref, ps_ref, oc_ref, os_ref = factor_refs
    rows = len(offsets)
    size = 32 // parts
    pitch = rows * 64 + 8
    lane = lane_index((size, 128))
    real = lane // 32 % 2 == 0
    back = lane // 32 * 32 + (32 - lane % 32) % 32
    slot = lane % 32 == 0
    groups = [[o for o in offsets if o % 2 == parity] for parity in range(2)]

    def tables_of(part):
        pc = pc_ref[part * size : part * size + size, :]
        ps = ps_ref[part * size : part * size + size, :]
        tables = []
        for group in groups:
            cosines = [pc * oc_ref[o : o + 1, :] - ps * os_ref[o : o + 1, :] for o in group]
            sines = [ps * oc_ref[o : o + 1, :] + pc * os_ref[o : o + 1, :] for o in group]
            tables.append(halves(jnp.concatenate(cosines + sines, axis=0)))
        return tables

    def products(tables, low, high):
        results = []
        for (t_high, t_low), g in zip(tables, (low + high, low - high)):
            g_high, g_low = halves(g)
            results.append(dot(t_high, g_high) + dot(t_low, g_high) + dot(t_high, g_low))
        return results

    def pieces(results, columns):
        for parity, group in enumerate(groups):
            count = len(group) * size
            for k, o in enumerate(group):
                p = results[parity][k * size : k * size + size, columns]
                q = results[parity][count + k * size : count + k * size + size, columns]
                turned = jnp.where(real, pltpu.roll(q, 96, 1), -pltpu.roll(q, 32, 1))
                other = p - turned
                yield offsets.index(o), p + turned, jnp.where(real, other, -other)

    def unpacked(start):
        blocks = []
        for s in range(start, start + 8):
            packed = g_ref[s, 256:EXT, :]
            for quarter in range(4):
                blocks.append(pltpu.roll(packed, 128 - 8 * quarter, 1) if quarter else packed)
        return jnp.concatenate(blocks, axis=0)

    for part in range(parts):
        tables = tables_of(part)
        ready(4, part)
        results = products(tables, unpacked(0), unpacked(8))
        extra = {k: m for k, _, m in pieces(results, slice(0, 128))}
        for pair in range(4):
            ready(pair, part)
            sides = []
            for start in (0, 8):
                columns = [
                    g_ref[start : start + 8, x2 * 32 : x2 * 32 + 32, :].reshape(256, 128)
                    for x2 in (2 * pair, 2 * pair + 1)
                ]
                sides.append(jnp.concatenate(columns, axis=1))
            results = products(tables, *sides)
            for x2 in (2 * pair, 2 * pair + 1):
                first = x2 % 2 * 128
                for k, direct, mirror in pieces(results, slice(first, first + 128)):
                    moved = pltpu.roll(extra[k], 128 - x2, 1) if x2 else extra[k]
                    mirror = jnp.where(slot, moved, mirror)
                    mirror = jnp.take_along_axis(mirror, back, axis=1)
                    at = x2 * pitch + k * 32 + part * size
                    stage_ref[at : at + size, :] = direct
                    stage_ref[at + rows * 32 : at + rows * 32 + size, :] = mirror
        deliver(part)


def y_kernel_a(offsets, g_ref, pc_ref, ps_ref, oc_ref, os_ref, target_ref, copy_ref, out_ref, stage_ref, copy_sem, out_sems):
    rows = len(offsets)
    pitch = rows * 64 + 8
    copy = pltpu.make_async_copy(g_ref, copy_ref, copy_sem)
    copy.start()

    def flush(part):
        window = pl.ds(part * 32, 32)
        return pltpu.make_async_copy(out_ref.at[window], target_ref.at[window], out_sems.at[part])

    def gather(p, carry):
        for pair in range(2):
            for k in range(rows):
                first = (pair * rows + k) * 32 + p
                block = stage_ref[pl.ds(first, 8, stride=pitch), :]
                out_ref[2 * p + pair, k * 8 : k * 8 + 8, :] = block
        return carry

    def deliver(part):
        for half in range(2):
            lax.fori_loop(half * 16, half * 16 + 16, gather, 0)
            flush(half).start()

    factors = (pc_ref, ps_ref, oc_ref, os_ref)
    y_rows(offsets, 1, g_ref, factors, stage_ref, lambda *_: None, deliver)
    copy.wait()
    flush(0).wait()
    flush(1).wait()


def y_kernel_b(offsets, core_ref, g_ref, pc_ref, ps_ref, oc_ref, os_ref, keep_ref, send_ref, stage_ref):
    rows = len(offsets)
    pitch = rows * 64 + 8
    core = core_ref[0]

    def gather(p, carry):
        for out_ref, side in ((keep_ref, core), (send_ref, 1 - core)):
            for pair in range(2):
                for k in range(rows):
                    first = (pair * rows + k) * 32 + 2 * p + side
                    block = stage_ref[pl.ds(first, 8, stride=pitch), :]
                    out_ref[2 * p + pair, k * 8 : k * 8 + 8, :] = block
        return carry

    def deliver(part):
        lax.fori_loop(0, 16, gather, 0)

    factors = (pc_ref, ps_ref, oc_ref, os_ref)
    y_rows(offsets, 1, g_ref, factors, stage_ref, lambda *_: None, deliver)


WHOLE = pl.BlockSpec(memory_space=pltpu.VMEM)
SMALL = pltpu.CompilerParams(vmem_limit_bytes=24 * 2**20)


def y_stage_a(blocks):
    rows = ROWS_A

    def kernel(*refs):
        y_kernel_a(list(range(ROWS_A)), *refs)

    hbm = pl.BlockSpec(memory_space=pltpu.HBM)
    return pl.pallas_call(
        kernel,
        in_specs=[WHOLE] * 5,
        out_specs=[hbm, hbm],
        out_shape=[
            pltpu.MemorySpace.HBM((64, rows * 8, 128), f32),
            pltpu.MemorySpace.HBM((16, EXT, 128), f32),
        ],
        scratch_shapes=[
            pltpu.VMEM((64, rows * 8, 128), f32),
            pltpu.VMEM((9 * (rows * 64 + 8), 128), f32),
            pltpu.SemaphoreType.DMA,
            pltpu.SemaphoreType.DMA((2,)),
        ],
        compiler_params=SMALL,
        name="y_stage_a",
        cost_estimate=pl.CostEstimate(flops=4 * 10**9, bytes_accessed=6 * 10**6, transcendentals=0),
    )(blocks, *y_factors())


def y_stage_b(core, blocks):
    rows = ROWS_B

    def kernel(*refs):
        y_kernel_b(list(range(ROWS_A, 16)), *refs)

    return pl.pallas_call(
        kernel,
        in_specs=[pl.BlockSpec(memory_space=pltpu.SMEM)] + [WHOLE] * 5,
        out_specs=[WHOLE, WHOLE],
        out_shape=[jax.ShapeDtypeStruct((32, rows * 8, 128), f32)] * 2,
        scratch_shapes=[pltpu.VMEM((9 * (rows * 64 + 8), 128), f32)],
        name="y_stage_b",
        cost_estimate=pl.CostEstimate(flops=4 * 10**9, bytes_accessed=6 * 10**6, transcendentals=0),
    )(core, blocks, *y_factors())


def x_tables(ac_ref, as_ref, bc_ref, bs_ref, high_ref, low_ref):
    for parity in range(2):
        bc = bc_ref[parity * 16 : parity * 16 + 16, :]
        bs = bs_ref[parity * 16 : parity * 16 + 16, :]
        for a in range(16):
            ac = ac_ref[a : a + 1, :]
            sa = as_ref[a : a + 1, :]
            full = jnp.concatenate([ac * bc - sa * bs, sa * bc + ac * bs], axis=1)
            high, low = halves(full)
            high_ref[parity, a * 16 : a * 16 + 16, :] = high
            low_ref[parity, a * 16 : a * 16 + 16, :] = low


def y_stage(blocks, offsets):
    offsets = list(offsets)
    rows = len(offsets)

    def kernel(*refs):
        y_kernel(offsets, *refs)

    whole = pl.BlockSpec(memory_space=pltpu.VMEM)
    hbm = pl.BlockSpec(memory_space=pltpu.HBM)
    return pl.pallas_call(
        kernel,
        in_specs=[hbm] + [whole] * 4,
        out_specs=hbm,
        out_shape=jax.ShapeDtypeStruct((64, rows * 8, 128), f32),
        scratch_shapes=[
            pltpu.VMEM((16, EXT, 128), f32),
            pltpu.VMEM((64, rows * 8, 128), f32),
            pltpu.VMEM((9 * (rows * 64 + 8), 128), f32),
            pltpu.SemaphoreType.DMA((5,)),
            pltpu.SemaphoreType.DMA((4,)),
        ],
        name=f"y_stage_{rows}",
        cost_estimate=pl.CostEstimate(flops=4 * 10**9, bytes_accessed=6 * 10**6, transcendentals=0),
    )(blocks, *y_factors())


def x_planes(high, g_ref, high_ref, low_ref, out_ref):
    turned = {}
    for o in range(STEP):
        for s in range(2):
            if len(g_ref.shape) == 5:
                block = g_ref[:, s, :, o * 8 : o * 8 + 8, :]
            else:
                block = g_ref[:, s, o * 8 : o * 8 + 8, :]
            block = block.reshape(256, 128)
            turned[o, s] = jnp.transpose(block)
    half = STEP * 64
    real = []
    imag = []
    for parity in range(2):
        rows = [
            turned[o, s][parity * 64 + part * 32 : parity * 64 + part * 32 + 32]
            for part in range(2)
            for o in range(STEP)
            for s in range(2)
        ]
        a_high, a_low = halves(jnp.concatenate(rows, axis=0))
        w_high = high_ref[parity]
        result = dot(a_high, w_high) + dot(a_low, w_high) + dot(a_high, low_ref[parity])
        real.append(result[:half, :256] + result[half:, 256:])
        imag.append(result[half:, :256] - result[:half, 256:])
    full_real = jnp.concatenate([real[0] + real[1], real[0] - real[1]], axis=1)
    full_imag = jnp.concatenate([imag[0] + imag[1], imag[0] - imag[1]], axis=1)
    for o in range(STEP):
        for s in range(2):
            base = pl.multiple_of(32 * jnp.bitwise_xor(high, s), 32)
            start = o * 64 + s * 32
            out_ref[0, o, pl.ds(base, 32), :] = full_real[start : start + 32]
            out_ref[1, o, pl.ds(base, 32), :] = full_imag[start : start + 32]


def fold(value):
    return value.reshape(8, 8, GRID).sum(axis=0)


def x_kernel_a(side_ref, y_ref, g_ref, ac_ref, as_ref, bc_ref, bs_ref, row_ref, col_ref, out_ref, sum_ref, acc_ref, high_ref, low_ref):
    step = pl.program_id(0)

    @pl.when(step == 0)
    def _():
        x_tables(ac_ref, as_ref, bc_ref, bs_ref, high_ref, low_ref)

    x_planes(side_ref[0], g_ref, high_ref, low_ref, out_ref)

    @pl.when(step == 0)
    def _():
        acc_ref[...] = jnp.zeros((7, 8, GRID), f32)

    mx = row_ref[0:1, :]
    mx_sq = row_ref[1:2, :]
    decay_x = row_ref[2:3, :]
    mx_back = row_ref[3:4, :]
    mod_x = row_ref[4:5, :]
    mod_x_back = row_ref[7:8, :]
    mz = col_ref[:, 0:1]
    mz_sq = col_ref[:, 1:2]
    decay_z = col_ref[:, 2:3]
    mz_back = col_ref[:, 3:4]
    mod_z = col_ref[:, 6:7]
    mod_z_back = col_ref[:, 9:10]
    for o in range(STEP):
        offset = step * STEP + o
        re = out_ref[0, o]
        im = out_ref[1, o]
        my = y_ref[0, offset]
        my_sq = y_ref[1, offset]
        decay_y = y_ref[2, offset]
        my_back = y_ref[3, offset]
        mod_y = y_ref[5, offset]
        paired = (offset >= 1) & (offset <= ROWS_B)
        mod_y_back = jnp.where(paired, y_ref[8, offset], 0.0)
        msq = mx_sq + (mz_sq + my_sq)
        anchor = msq == 0.0
        inverse = 1.0 / jnp.where(anchor, 1.0, msq)
        decay = decay_x * (decay_z * (decay_y * (1.0 / (math.pi * VOLUME))))
        base = decay * inverse * (re * re + im * im)
        base = jnp.where(anchor, 0.0, base)
        first = base * (mod_x * (mod_z * mod_y))
        second = base * (mod_x_back * (mod_z_back * mod_y_back))
        factor = (1.0 + RATE * msq) * inverse
        t1 = first * factor
        t2 = second * factor
        s1 = fold(t1)
        s2 = fold(t2)
        both = s1 + s2
        z1 = fold(t1 * mz)
        z2 = fold(t2 * mz_back)
        acc_ref[0] += fold(first + second)
        acc_ref[1] += both * mx_sq
        acc_ref[2] += both * my_sq
        acc_ref[3] += fold((t1 + t2) * mz_sq)
        acc_ref[4] += s1 * (mx * my) + s2 * (mx_back * my_back)
        acc_ref[5] += z1 * mx + z2 * mx_back
        acc_ref[6] += z1 * my + z2 * my_back

    @pl.when(step == pl.num_programs(0) - 1)
    def _():
        total = acc_ref[...]
        total = total[:, :, :128] + total[:, :, 128:256] + total[:, :, 256:384] + total[:, :, 384:]
        totals = jnp.sum(total.sum(axis=1), axis=1, keepdims=True)
        energy = 0.5 * totals[0:1]
        sum_ref[0:1, :] = jnp.broadcast_to(energy, (1, 128))
        sum_ref[1:4, :] = jnp.broadcast_to(energy - totals[1:4], (3, 128))
        sum_ref[4:7, :] = jnp.broadcast_to(-totals[4:7], (3, 128))
        sum_ref[7:8, :] = jnp.zeros((1, 128), f32)


def x_kernel_b(side_ref, g_ref, ac_ref, as_ref, bc_ref, bs_ref, whole_ref, out_ref, high_ref, low_ref):
    del whole_ref

    @pl.when(pl.program_id(0) == 0)
    def _():
        x_tables(ac_ref, as_ref, bc_ref, bs_ref, high_ref, low_ref)

    x_planes(side_ref[0], g_ref, high_ref, low_ref, out_ref)


FACTORS = [pl.BlockSpec((rows, 256), lambda i: (0, 0)) for rows in (16, 16, 32, 32)]
TABLES = [pltpu.VMEM((2, 256, GRID), bf16)] * 2
OUT_SHAPE = jax.ShapeDtypeStruct((2, 16, 64, GRID), f32)


def x_stage_a(side, y_numbers, blocks, row_numbers, col_numbers):
    smem = pl.BlockSpec(memory_space=pltpu.SMEM)
    return pl.pallas_call(
        x_kernel_a,
        grid=(ROWS_A // STEP,),
        in_specs=[
            smem,
            smem,
            pl.BlockSpec((32, 2, STEP * 8, 128), lambda i: (0, 0, i, 0)),
            *FACTORS,
            pl.BlockSpec((10, GRID), lambda i: (0, 0)),
            pl.BlockSpec((64, 10), lambda i: (0, 0)),
        ],
        out_specs=[
            pl.BlockSpec((2, STEP, 64, GRID), lambda i: (0, i, 0, 0)),
            pl.BlockSpec((8, 128), lambda i: (0, 0)),
        ],
        out_shape=[OUT_SHAPE, jax.ShapeDtypeStruct((8, 128), f32)],
        scratch_shapes=[pltpu.VMEM((7, 8, GRID), f32), *TABLES],
        compiler_params=pltpu.CompilerParams(vmem_limit_bytes=24 * 2**20),
        name="x_stage_a",
        cost_estimate=pl.CostEstimate(flops=4 * 10**9, bytes_accessed=6 * 10**6, transcendentals=0),
    )(side, y_numbers, blocks, *x_factors(), row_numbers, col_numbers)


def x_stage_b(side, blocks, whole):
    smem = pl.BlockSpec(memory_space=pltpu.SMEM)
    return pl.pallas_call(
        x_kernel_b,
        grid=(ROWS_B // STEP,),
        in_specs=[
            smem,
            pl.BlockSpec((16, 2, 2, STEP * 8, 128), lambda i: (0, 0, 0, i, 0)),
            *FACTORS,
            pl.BlockSpec(memory_space=pl.ANY),
        ],
        out_specs=pl.BlockSpec((2, STEP, 64, GRID), lambda i: (0, ROWS_A // STEP + i, 0, 0)),
        out_shape=OUT_SHAPE,
        scratch_shapes=TABLES,
        input_output_aliases={6: 0},
        compiler_params=pltpu.CompilerParams(vmem_limit_bytes=24 * 2**20),
        name="x_stage_b",
        cost_estimate=pl.CostEstimate(flops=4 * 10**9, bytes_accessed=6 * 10**6, transcendentals=0),
    )(side, blocks, *x_factors(), whole)


def pair_groups(split_cores):
    ids = np.arange(256).reshape(16, 2, 8)
    groups = []
    for q in range(4):
        members = np.stack([ids[:, :, q], ids[:, :, 7 - q]], axis=2)
        if split_cores:
            groups += [members[:, core].reshape(-1).tolist() for core in range(2)]
        else:
            groups.append(members.reshape(-1).tolist())
    return groups


def exchange(blocks, split_cores):
    return lax.all_to_all(
        blocks, ALL, split_axis=0, concat_axis=0, tiled=True, axis_index_groups=pair_groups(split_cores)
    )


def all_sum(value):
    for axis in (("px_2",), ("px_0",), ("py_1",), ("px_1",), ("py_0",)):
        size = lax.axis_size(axis)
        parts = [value]
        for k in range(1, size):
            parts.append(lax.ppermute(value, axis, [(s, s ^ k) for s in range(size)]))
        while len(parts) > 1:
            parts = [a + b for a, b in zip(parts[::2], parts[1::2])]
        value = parts[0]
    return value


def body(charges_old, spline_moduli):
    row_position = lax.axis_index(PX)
    col_position = lax.axis_index(PY)
    side = (col_position >= 4).astype(jnp.int32)
    planes = z_stage(charges_old[0, 0], z_table())
    planes = lax.all_to_all(planes, FIRST, split_axis=0, concat_axis=0, tiled=True)

    backward = jnp.roll(jnp.flip(spline_moduli, axis=1), 1, axis=1)
    numbers = jnp.concatenate([jnp.asarray(wave_rows()), spline_moduli, backward])
    col_numbers = lax.dynamic_slice_in_dim(numbers, col_position * 64, 64, axis=1).T
    y_numbers = lax.dynamic_slice_in_dim(numbers, row_position * 16, 16, axis=1)

    part_a, planes = y_stage_a(planes)
    part_a = exchange(part_a, False).reshape(32, 2, ROWS_A * 8, 128)
    planes, numbers, col_numbers, y_numbers = lax.optimization_barrier(
        (planes, numbers, col_numbers, y_numbers)
    )
    core = lax.axis_index("px_2")
    keep, send = y_stage_b(core.reshape(1), planes)
    received = lax.ppermute(send, "px_2", [(0, 1), (1, 0)])
    lower = core == 0
    halves_of_x = [jnp.where(lower, keep, received), jnp.where(lower, received, keep)]
    part_b = exchange(jnp.stack(halves_of_x, axis=1), True).reshape(16, 2, 2, ROWS_B * 8, 128)

    whole, sums = x_stage_a(side.reshape(1), y_numbers, part_a, numbers, col_numbers)
    sums = all_sum(sums)
    structure = x_stage_b(side.reshape(1), part_b, whole)
    return structure, sums[0, 0], sums[1:7, 0]


def solution(mesh):
    torus = Mesh(mesh.devices.reshape(4, 4, 2, 2, 4), ALL)
    return jax.shard_map(
        body,
        mesh=torus,
        in_specs=(P(PX, PY, None, None, None), P()),
        out_specs=(P(None, PX, PY, None), P(), P()),
        check_vma=False,
    )
```
